32 devices in a mesh: energy: 16 (over z, x, core), mode: 2 (over y).
Axes of the slice: x: 2, y: 2, z: 4, core: 2. Of those that a mesh axis runs over, the one named last changes fastest.
Arguments:
- spectral: float32 [16, 896, 896], P('energy', 'mode'), may hold values from -6 to 6
- coupling: bfloat16 [2, 896, 896], P('mode'), may hold values from -0.1875 to 0.1875
- offsets: int32 [2], P('mode'), may hold values from 1 to 2, as said below
- occupation: int32 [2, 16], P('mode', 'energy'), may hold values from 0 to 3
Outputs:
- self_energy: float32 [16, 896, 896], P('energy', 'mode')
The draws below stay inside these ranges and needn't reach their ends.
Inputs may be any that keep to these rules, and one draw needn't show every extreme that they name: `offsets`: each offset from 1 to 2 belongs to exactly 1 modes.
All inputs are finite; a program needn't handle non-finite values.
Results may differ from the reference program's by a relative error of at most 0.0041.
Values sent between devices are 32-bit elements; how exact they have to be, the bound alone decides.
No kernel may reach another device: no remote copies, remote signals or barrier semaphores. Data moves between devices by JAX's collectives and lax.ppermute only.
A program may use at most 64 MiB of HBM per device.

```python
import jax
import jax.numpy as jnp
from jax import lax

NORB = 896
KMAX = 2
ENERGIES = 16
MODES = 2


def draw_offsets(key, part):
    shuffled = jax.random.permutation(jax.random.fold_in(key, 11), MODES)
    return (1 + shuffled % KMAX).astype(jnp.int32)


def with_ends(drawn, key, low, top_value):
    spot = [jax.random.randint(jax.random.fold_in(key, axis), (), 0, length) for axis, length in enumerate(drawn.shape)]
    longest = drawn.shape.index(max(drawn.shape))
    beside = spot[:longest] + [(spot[longest] + 1) % drawn.shape[longest]] + spot[longest + 1:]
    return drawn.at[tuple(spot)].set(low).at[tuple(beside)].set(top_value)


def block_levels(key, extent, cuts, low, high):
    level = 1.0
    for position, parts in cuts:
        steps = jax.random.uniform(jax.random.fold_in(jax.random.fold_in(key, 6), position), (parts,), jnp.float32, low / len(cuts), high / len(cuts))
        level = level * jnp.repeat(jnp.exp(steps), extent[position] // parts).reshape((-1,) + (1,) * (len(extent) - 1 - position))
    return level


def normal_values(stream_key, dims, deviation, bound, shards=(), kind=jnp.bfloat16):
    entries = jax.random.normal(stream_key, dims, jnp.float32) * deviation
    if len(shards) > 0:
        entries = block_levels(stream_key, dims, shards, -0.22, 0.18) * entries
    return jnp.clip(entries, min=-bound, max=bound).astype(kind)


def setup_inputs(seed: int = 0) -> dict:
    keys = jax.random.split(jax.random.key(seed), 5)
    spectral = normal_values(keys[0], (ENERGIES, NORB, NORB), 1.0, 6.0, ((0, 16), (1, 2)), jnp.float32)
    coupling = normal_values(keys[1], (MODES, NORB, NORB), NORB ** -0.5, 0.1875, ((0, 2),))
    offsets = draw_offsets(jax.random.fold_in(keys[4], 71), 0)
    occupation = with_ends(jax.random.randint(keys[3], (MODES, ENERGIES), 0, 4), jax.random.fold_in(keys[3], 1), 0, 3).astype(jnp.int32)
    return dict(spectral=spectral, coupling=coupling, offsets=offsets, occupation=occupation)


def reference(spectral, coupling, offsets, occupation):
    energies = spectral.shape[0]
    padded = jnp.pad(spectral, ((KMAX, KMAX), (0, 0), (0, 0)))
    energy_index = jnp.arange(energies, dtype=jnp.int32)

    def one_mode(running, inputs):
        matrix, offset, occupied = inputs
        emitted = jnp.take(padded, energy_index + KMAX - offset, axis=0)
        absorbed = jnp.take(padded, energy_index + KMAX + offset, axis=0)
        emission = (occupied + 1).astype(jnp.float32)[:, None, None]
        absorption = occupied.astype(jnp.float32)[:, None, None]
        combined = (emission * emitted + absorption * absorbed).astype(jnp.bfloat16)
        matrix_wide = matrix.astype(jnp.float32)
        coupled = jnp.einsum("ij,ejk->eik", matrix_wide, combined.astype(jnp.float32)).astype(jnp.bfloat16)
        mode_term = jnp.einsum("eik,lk->eil", coupled.astype(jnp.float32), matrix_wide)
        return running + mode_term, None

    start_value = jnp.zeros(spectral.shape, jnp.float32)
    running, unused = lax.scan(one_mode, start_value, (coupling, offsets, occupation))
    return running / MODES
```

```python
import functools

import jax
import jax.numpy as jnp
from jax import lax
from jax.experimental import pallas as pl
from jax.experimental.pallas import tpu as pltpu
from jax.sharding import PartitionSpec as P


VMEM = pl.BlockSpec(memory_space=pltpu.VMEM)
SMEM = pl.BlockSpec(memory_space=pltpu.SMEM)
LOCAL_BYTES = 12 * 2**20
SWAP = [(0, 1), (1, 0)]
INPUT_WIDTH = 256
OUTPUT_CUTS = (256,)


def cuts(extent, width):
    return [(start, min(start + width, extent)) for start in range(0, extent, width)]


def permute_energy(value, target_of):
    count = lax.axis_size("energy")
    pairs = [(source, target_of(source)) for source in range(count)]
    pairs = [(source, target) for source, target in pairs if target is not None and 0 <= target < count]
    return lax.ppermute(value, "energy", pairs)


def partner(energy):
    return energy ^ 1


def across(energy):
    return energy ^ 2


def onward(energy):
    return energy + 4 if energy & 2 == 0 else energy - 4


def straight(energy):
    return energy ^ 1 if (energy >> 1) & 1 == energy & 1 else None


def crossed(energy):
    return energy ^ 1 if (energy >> 1) & 1 != energy & 1 else None


def local_call(kernel, outputs, scalars, arrays):
    held = [pltpu.with_memory_space_constraint(each, pltpu.VMEM) for each in arrays]
    return pl.pallas_call(
        kernel,
        out_shape=[pltpu.VMEM(shape, dtype) for shape, dtype in outputs],
        in_specs=[SMEM] * len(scalars) + [VMEM] * len(held),
        out_specs=[VMEM] * len(outputs),
        compiler_params=pltpu.CompilerParams(vmem_limit_bytes=LOCAL_BYTES),
    )(*scalars, *held)


def take_columns(matrix_ref, out_ref):
    rows = out_ref.shape[1]
    mode = lax.axis_index("mode")

    @pl.when(mode == 0)
    def _():
        out_ref[...] = matrix_ref[:, :rows]

    @pl.when(mode != 0)
    def _():
        out_ref[...] = matrix_ref[:, rows:]


def cut_kernel(columns, own_ref, *refs):
    pieces, sem = refs[:-1], refs[-1]
    copies = [
        pltpu.make_async_copy(own_ref.at[0, :, first:last], piece, sem.at[index])
        for index, ((first, last), piece) in enumerate(zip(columns, pieces))
    ]
    for copy in copies:
        copy.start()
    for copy in copies:
        copy.wait()


def widen_kernel(offset_ref, level_ref, matrix_ref, wide_ref, numbers_ref):
    rows = wide_ref.shape[0]
    core = lax.axis_index("energy") & 1
    wide_ref[...] = matrix_ref[pl.ds(pl.multiple_of(core * rows, rows), rows), :].astype(wide_ref.dtype)
    row = lax.broadcasted_iota(jnp.int32, numbers_ref.shape, 0)
    numbers_ref[...] = jnp.where(row == 0, offset_ref[0], level_ref[0, 0])


def columns_kernel(matrix_ref, out_ref):
    take_columns(matrix_ref, out_ref)


def join_kernel(mine_ref, other_ref, out_ref, left_ref):
    rows = mine_ref.shape[0]
    core = lax.axis_index("energy") & 1
    out_ref[pl.ds(pl.multiple_of(core * rows, rows), rows), :] = mine_ref[...].astype(out_ref.dtype)
    out_ref[pl.ds(pl.multiple_of((1 - core) * rows, rows), rows), :] = other_ref[...].astype(out_ref.dtype)
    take_columns(out_ref, left_ref)


def left_kernel(columns, partner_ref, across_ref, onward_ref, straight_ref, crossed_ref, *refs):
    modes = len(refs) // 3
    numbers, lefts, outs = refs[:modes], refs[modes : 2 * modes], refs[2 * modes :]
    energy = lax.axis_index("energy")
    step = 1 - 2 * (energy & 1)
    far = 2 - 4 * ((energy >> 1) & 1)
    sources = (
        (partner_ref[:, columns[0] : columns[1]], step),
        (across_ref[...], far),
        (onward_ref[...], -far),
        (straight_ref[...] + crossed_ref[...], -step),
    )
    for number, left, out in zip(numbers, lefts, outs):
        offset, level = number[0:1, 0:1], number[1:2, 0:1]
        total = None
        for source, distance in sources:
            below = jnp.where(distance < 0, 1, 0)
            weight = jnp.where(offset == jnp.abs(distance), level + below, 0).astype(jnp.float32)
            total = source * weight if total is None else total + source * weight
        product = jnp.dot(left[...], total.astype(jnp.bfloat16), preferred_element_type=jnp.float32)
        out[...] = product.astype(jnp.bfloat16)


def right_kernel(scale, columns, targets, away, *refs):
    modes = 2
    out_ref = refs[-1]
    couplings = refs[:modes]
    pieces = refs[modes:-1]
    rows = out_ref.shape[0]
    mode = lax.axis_index("mode")
    start = pl.multiple_of((1 - mode if away else mode) * rows, rows)
    low, high = targets
    total = None
    for mode in range(modes):
        for index, (first, last) in enumerate(columns):
            left = pieces[mode * len(columns) + index][pl.ds(start, rows), :]
            term = lax.dot_general(
                left,
                couplings[mode][low:high, first:last],
                (((1,), (1,)), ((), ())),
                preferred_element_type=jnp.float32,
            )
            total = term if total is None else total + term
    out_ref[...] = total * scale


def shards(spectral, coupling, offsets, occupation):
    rows, orbitals = spectral.shape[1:]
    matrix = coupling[0]
    modes = lax.axis_size("mode")
    columns = cuts(orbitals, INPUT_WIDTH)

    own_piece = pl.pallas_call(
        functools.partial(cut_kernel, columns),
        out_shape=[pltpu.VMEM((rows, last - first), jnp.float32) for first, last in columns],
        in_specs=[pl.BlockSpec(memory_space=pl.ANY)],
        out_specs=[VMEM] * len(columns),
        scratch_shapes=[pltpu.SemaphoreType.DMA((len(columns),))],
        compiler_params=pltpu.CompilerParams(vmem_limit_bytes=LOCAL_BYTES),
        name="cut",
    )(spectral)
    across_piece, onward_piece, straight_piece, crossed_piece = [], [], [], []
    for index in range(len(columns)):
        across_piece.append(permute_energy(own_piece[index], across))

    wide, numbers = local_call(
        widen_kernel, [((orbitals // 2, orbitals), jnp.float32), ((8, 128), jnp.int32)], [offsets, occupation], [matrix]
    )
    half_mine = lax.ppermute(wide, "mode", SWAP)
    half_other = permute_energy(half_mine, partner)
    other_numbers = lax.ppermute(numbers, "mode", SWAP)
    partner_piece = permute_energy(spectral[0], partner)

    for index in range(len(columns)):
        onward_piece.append(permute_energy(across_piece[index], onward))
        straight_piece.append(permute_energy(across_piece[index], straight))
        crossed_piece.append(permute_energy(onward_piece[index], crossed))

    left_shape = ((orbitals, rows), matrix.dtype)
    (own_left,) = local_call(columns_kernel, [left_shape], [], [matrix])
    other_matrix, other_left = local_call(
        join_kernel, [(matrix.shape, matrix.dtype), left_shape], [], [half_mine, half_other]
    )
    matrices = (matrix, other_matrix)

    pieces = [[], []]
    for index, (first, last) in enumerate(columns):
        results = local_call(
            functools.partial(left_kernel, (first, last)),
            [((orbitals, last - first), jnp.bfloat16)] * 2,
            [],
            [
                partner_piece,
                across_piece[index],
                onward_piece[index],
                straight_piece[index],
                crossed_piece[index],
                numbers,
                other_numbers,
                own_left,
                other_left,
            ],
        )
        for mode_index in range(2):
            pieces[mode_index].append(results[mode_index])

    def right(away, targets):
        (result,) = local_call(
            functools.partial(right_kernel, 1.0 / modes, columns, targets, away),
            [((rows, targets[1] - targets[0]), jnp.float32)],
            [],
            [*matrices, *pieces[0], *pieces[1]],
        )
        return result

    bounds = (0, *OUTPUT_CUTS, orbitals)
    arrived = []
    for targets in zip(bounds[:-1], bounds[1:]):
        sent = right(True, targets)
        arrived.append(lax.ppermute(sent, "mode", SWAP))
    kept = right(False, (0, orbitals))
    return (kept + jnp.concatenate(arrived, axis=1))[None]


def solution(mesh):
    return jax.shard_map(
        shards,
        mesh=mesh,
        in_specs=(P("energy", "mode", None), P("mode", None, None), P("mode"), P("mode", "energy")),
        out_specs=P("energy", "mode", None),
        check_vma=False,
    )
```

```python
import functools

import jax
import jax.numpy as jnp
from jax import lax
from jax.experimental import pallas as pl
from jax.experimental.pallas import tpu as pltpu
from jax.sharding import PartitionSpec as P


VMEM = pl.BlockSpec(memory_space=pltpu.VMEM)
SMEM = pl.BlockSpec(memory_space=pltpu.SMEM)
LOCAL_BYTES = 12 * 2**20
SWAP = [(0, 1), (1, 0)]
WIDTH = 256
OUT_FIRST = 256
SECOND = ((0, 1), (1, 2), (2, 4))


def cuts(extent, width):
    return [(start, min(start + width, extent)) for start in range(0, extent, width)]


def detour(energy):
    return energy - 4 if energy & 2 == 0 else energy + 4


def is_early(energy):
    return (energy ^ (energy >> 1)) & 1


def permute_energy(value, target_of, early=None):
    count = lax.axis_size("energy")
    pairs = [(source, target_of(source)) for source in range(count) if early is None or is_early(source) == early]
    return lax.ppermute(value, "energy", [(source, target) for source, target in pairs if 0 <= target < count])


def permute_mode(value, early):
    count, modes = lax.axis_size("energy"), lax.axis_size("mode")
    pairs = [
        (energy * modes + mode, energy * modes + other)
        for energy in range(count)
        if is_early(energy) == early
        for mode, other in SWAP
    ]
    return lax.ppermute(value, ("energy", "mode"), pairs)


def partner(energy):
    return energy ^ 1


def across(energy):
    return energy ^ 2


def onward(energy):
    return energy + 4 if energy & 2 == 0 else energy - 4


def local_call(kernel, outputs, scalars, arrays):
    held = [pltpu.with_memory_space_constraint(each, pltpu.VMEM) for each in arrays]
    return pl.pallas_call(
        kernel,
        out_shape=[pltpu.VMEM(shape, dtype) for shape, dtype in outputs],
        in_specs=[SMEM] * len(scalars) + [VMEM] * len(held),
        out_specs=[VMEM] * len(outputs),
        compiler_params=pltpu.CompilerParams(vmem_limit_bytes=LOCAL_BYTES),
    )(*scalars, *held)


def take_columns(matrix_ref, out_ref):
    rows = out_ref.shape[1]
    mode = lax.axis_index("mode")

    @pl.when(mode == 0)
    def _():
        out_ref[...] = matrix_ref[:, :rows]

    @pl.when(mode != 0)
    def _():
        out_ref[...] = matrix_ref[:, rows:]


def cut_kernel(columns, own_ref, *refs):
    pieces, sem = refs[:-1], refs[-1]
    copies = [
        pltpu.make_async_copy(own_ref.at[0, :, first:last], piece, sem.at[index])
        for index, ((first, last), piece) in enumerate(zip(columns, pieces))
    ]
    for copy in copies:
        copy.start()
    for copy in copies:
        copy.wait()


def merge_kernel(*refs):
    at = 0
    for piece in refs[:-1]:
        width = piece.shape[1]
        refs[-1][:, at : at + width] = piece[...]
        at += width


def part_of(matrix_ref, part, index):
    at = ((lax.axis_index("energy") & 1) * 2 + index) * part
    return matrix_ref[pl.ds(pl.multiple_of(at, part), part), :]


def widen_kernel(matrix_ref, out_ref):
    out_ref[...] = part_of(matrix_ref, out_ref.shape[0], 0).astype(out_ref.dtype)


def widen_more_kernel(offset_ref, level_ref, matrix_ref, out_ref):
    orbitals = matrix_ref.shape[0]
    part = orbitals // 4
    out_ref[0:part, :] = part_of(matrix_ref, part, 1).astype(out_ref.dtype)
    row = lax.broadcasted_iota(jnp.int32, (out_ref.shape[0] - part, orbitals), 0)
    out_ref[part:, :] = jnp.where(row == 0, offset_ref[0], level_ref[0, 0]).astype(out_ref.dtype)


def columns_kernel(matrix_ref, out_ref):
    take_columns(matrix_ref, out_ref)


def join_kernel(*refs):
    halves, (out_ref, left_ref) = refs[:-2], refs[-2:]
    part = out_ref.shape[0] // 4
    core = lax.axis_index("energy") & 1
    for index, half in enumerate(halves):
        owner = core if index < 2 else 1 - core
        at = pl.multiple_of((2 * owner + index % 2) * part, part)
        out_ref[pl.ds(at, part), :] = half[0:part, :].astype(out_ref.dtype)
    take_columns(out_ref, left_ref)


def piece_view(refs, starts, first, last):
    for ref, start in zip(refs, starts):
        if start <= first and last <= start + ref.shape[1]:
            return ref[:, first - start : last - start]
    raise ValueError((first, last, starts))


def left_kernel(tiles, layout, early, number, left, *refs):
    out, combined = refs[-2:]
    rows = combined.shape[0]
    split, at = [], 0
    for starts in layout:
        split.append((refs[at : at + len(starts)], starts))
        at += len(starts)
    energy = lax.axis_index("energy")

    @pl.when(is_early(energy) == early)
    def _():
        step = 1 - 2 * (energy & 1)
        far = 2 - 4 * ((energy >> 1) & 1)
        told = left.shape[0] // 4
        start = pl.multiple_of((1 - lax.axis_index("mode")) * rows, rows)
        offset, level = number[told : told + 1, 0:1], number[told + 1 : told + 2, 0:1]

        def weight(distance):
            gap = jnp.abs(distance).astype(jnp.float32)
            below = jnp.where(distance < 0, 1, 0).astype(jnp.float32)
            return jnp.where(offset == gap, level + below, 0.0)

        weights = [weight(distance) for distance in (step, far, -far, -step)]
        for first, last in tiles:
            total = None
            for (pieces, starts), factor in zip(split, weights):
                term = piece_view(pieces, starts, first, last) * factor
                total = term if total is None else total + term
            total = total.astype(jnp.bfloat16)
            span = slice(first - tiles[0][0], last - tiles[0][0])
            combined[:, span] = total
            product = jnp.dot(left[pl.ds(start, rows), :], total, preferred_element_type=jnp.float32)
            out[:, span] = product.astype(jnp.bfloat16)


def right_product(couplings, pieces, columns, targets):
    low, high = targets
    total = None
    for coupling, lefts in zip(couplings, pieces):
        for left, (first, last) in zip(lefts, columns):
            term = lax.dot_general(
                left, coupling[low:high, first:last], (((1,), (1,)), ((), ())), preferred_element_type=jnp.float32
            )
            total = term if total is None else total + term
    return total


def send_kernel(scale, columns, targets, early, *refs):
    pieces, out_ref = refs[2:-1], refs[-1]
    many = len(columns)

    @pl.when(is_early(lax.axis_index("energy")) == early)
    def _():
        lefts = [[piece[...] for piece in pieces[mode * many : (mode + 1) * many]] for mode in range(2)]
        out_ref[...] = right_product(refs[:2], lefts, columns, targets) * scale


def keep_kernel(scale, columns, targets, *refs):
    couplings, lefts, out_ref = refs[:2], refs[2:4], refs[-1]
    rows = out_ref.shape[0]
    start = pl.multiple_of(lax.axis_index("mode") * rows, rows)
    many = len(columns)
    for early in range(2):
        pieces = refs[4 + 2 * many * early : 4 + 2 * many * (early + 1)]

        @pl.when(is_early(lax.axis_index("energy")) == early)
        def _(pieces=pieces):
            held = [
                [
                    jnp.dot(
                        left[pl.ds(start, rows), :], piece[...], preferred_element_type=jnp.float32
                    ).astype(jnp.bfloat16)
                    for piece in pieces[mode * many : (mode + 1) * many]
                ]
                for mode, left in enumerate(lefts)
            ]
            out_ref[...] = right_product(couplings, held, columns, targets) * scale


def finish_kernel(columns, *refs):
    kept_ref, early_ref, late_ref = refs[:3]
    out_ref, total_ref, sem = refs[-3:]
    first, last = columns
    total_ref[...] = kept_ref[:, first:last] + (early_ref[...] + late_ref[...])
    copy = pltpu.make_async_copy(total_ref, out_ref.at[0, :, first:last], sem)
    copy.start()
    copy.wait()


def finish(columns, kept, early, late, before):
    rows, orbitals = kept.shape
    held = [pltpu.with_memory_space_constraint(each, pltpu.VMEM) for each in (kept, early, late)]
    return pl.pallas_call(
        functools.partial(finish_kernel, columns),
        out_shape=jax.ShapeDtypeStruct((1, rows, orbitals), kept.dtype),
        in_specs=[VMEM] * 3 + [pl.BlockSpec(memory_space=pl.ANY)] * len(before),
        out_specs=pl.BlockSpec(memory_space=pl.ANY),
        scratch_shapes=[pltpu.VMEM((rows, columns[1] - columns[0]), kept.dtype), pltpu.SemaphoreType.DMA],
        input_output_aliases={3: 0} if before else {},
        compiler_params=pltpu.CompilerParams(vmem_limit_bytes=LOCAL_BYTES),
        name="finish",
    )(*held, *before)


def cut(spectral, columns):
    return pl.pallas_call(
        functools.partial(cut_kernel, columns),
        out_shape=[pltpu.VMEM((spectral.shape[1], last - first), jnp.float32) for first, last in columns],
        in_specs=[pl.BlockSpec(memory_space=pl.ANY)],
        out_specs=[VMEM] * len(columns),
        scratch_shapes=[pltpu.SemaphoreType.DMA((len(columns),))],
        compiler_params=pltpu.CompilerParams(vmem_limit_bytes=LOCAL_BYTES),
    )(spectral)


def merged(pieces):
    if len(pieces) == 1:
        return pieces[0]
    rows = pieces[0].shape[0]
    return local_call(merge_kernel, [((rows, sum(each.shape[1] for each in pieces)), jnp.float32)], [], pieces)[0]


def shards(spectral, coupling, offsets, occupation):
    rows, orbitals = spectral.shape[1:]
    matrix = coupling[0]
    scale = 1.0 / lax.axis_size("mode")
    tiles = cuts(orbitals, WIDTH)
    half = len(tiles) // 2
    sides = ((0, half), (half, len(tiles)))

    own_piece = cut(spectral, tiles[:1])
    across_piece = [permute_energy(own_piece[0], across)]
    own_piece += cut(spectral, tiles[1:])
    for index in range(1, len(tiles)):
        across_piece.append(permute_energy(own_piece[index], across))

    part = orbitals // 4
    (wide,) = local_call(widen_kernel, [((part, orbitals), jnp.float32)], [], [matrix])
    (wide_rest,) = local_call(widen_more_kernel, [((part + 8, orbitals), jnp.float32)], [offsets, occupation], [matrix])
    told = lax.ppermute(wide, "mode", SWAP)
    told_rest = lax.ppermute(wide_rest, "mode", SWAP)
    swapped = permute_energy(told, partner)
    swapped_rest = permute_energy(told_rest, partner)
    partner_piece = permute_energy(spectral[0], partner)

    first_piece = []
    for index in range(len(tiles) - 1):
        first_piece.append(permute_energy(across_piece[index], onward, early=1))
    aside = permute_energy(own_piece[-1], detour, early=0)
    first_piece.append(permute_energy(aside, across, early=0))
    second_piece = []
    for low, high in SECOND:
        second_piece.append(permute_energy(merged(across_piece[low:high]), onward, early=0))
    straight_piece = []
    for low, high in sides:
        straight_piece.append(permute_energy(merged(across_piece[low:high]), partner, early=0))
    crossed_piece = permute_energy(merged(first_piece), partner, early=1)

    left_shape = ((orbitals, rows), matrix.dtype)
    (own_left,) = local_call(columns_kernel, [left_shape], [], [matrix])
    other_matrix, other_left = local_call(
        join_kernel, [(matrix.shape, matrix.dtype), left_shape], [], [told, told_rest, swapped, swapped_rest]
    )
    matrices = (matrix, other_matrix)

    starts = [first for first, last in tiles]

    def left(which, low, high, early, onward_pieces, onward_starts, back_piece, back_start):
        number, columns = ((wide_rest, own_left), (told_rest, other_left))[which]
        layout = ([0], starts[low:high], onward_starts, [back_start])
        width = tiles[high - 1][1] - tiles[low][0]
        return local_call(
            functools.partial(left_kernel, tiles[low:high], layout, early),
            [((rows, width), jnp.bfloat16)] * 2,
            [],
            [number, columns, partner_piece, *across_piece[low:high], *onward_pieces, back_piece],
        )

    early_pieces, late_pieces = [], []
    for which in range(2):
        for index, (low, high) in enumerate(sides):
            early_pieces.append(
                left(
                    which, low, high, 1,
                    first_piece[low:high], starts[low:high], straight_piece[index], starts[low],
                )
            )
            seconds = [each for each, (begin, end) in enumerate(SECOND) if low <= begin and end <= high]
            late_pieces.append(
                left(
                    which, low, high, 0,
                    [second_piece[each] for each in seconds], [starts[SECOND[each][0]] for each in seconds],
                    crossed_piece, 0,
                )
            )
    columns = [(tiles[low][0], tiles[high - 1][1]) for low, high in sides]

    bounds = ((0, OUT_FIRST), (OUT_FIRST, orbitals))
    arrived = []
    for early, pieces in ((1, early_pieces), (0, late_pieces)):
        got = []
        for targets in bounds:
            (sent,) = local_call(
                functools.partial(send_kernel, scale, columns, targets, early),
                [((rows, targets[1] - targets[0]), jnp.float32)],
                [],
                [*matrices, *(left for left, combined in pieces)],
            )
            got.append(permute_mode(sent, early))
        arrived.append(got)
    combined = [each for pieces in (late_pieces, early_pieces) for left, each in pieces]
    (kept,) = local_call(
        functools.partial(keep_kernel, scale, columns, (0, orbitals)),
        [((rows, orbitals), jnp.float32)],
        [],
        [*matrices, own_left, other_left, *combined],
    )
    result = []
    for index, targets in enumerate(bounds):
        result = [finish(targets, kept, arrived[0][index], arrived[1][index], result)]
    return result[0]


def solution(mesh):
    return jax.shard_map(
        shards,
        mesh=mesh,
        in_specs=(P("energy", "mode", None), P("mode", None, None), P("mode"), P("mode", "energy")),
        out_specs=P("energy", "mode", None),
        check_vma=False,
    )
```

```python
import functools

import jax
import jax.numpy as jnp
from jax import lax
from jax.experimental import pallas as pl
from jax.experimental.pallas import tpu as pltpu
from jax.sharding import PartitionSpec as P


ANY = pl.BlockSpec(memory_space=pl.ANY)
VMEM = pl.BlockSpec(memory_space=pltpu.VMEM)
SMEM = pl.BlockSpec(memory_space=pltpu.SMEM)
LOCAL = pltpu.CompilerParams(vmem_limit_bytes=12 * 2**20)
SWAP = [(0, 1), (1, 0)]
LANES = 128


def tiles_of(columns):
    tiles, first = [], 0
    while first < columns:
        last = min(columns, first + (2 * LANES if columns - first > 3 * LANES else LANES))
        tiles.append((first, last))
        first = last
    return tiles


def is_early(energy):
    return (energy ^ (energy >> 1)) & 1


def partner(energy):
    return energy ^ 1


def across(energy):
    return energy ^ 2


def onward(energy):
    return energy + 4 if energy & 2 == 0 else energy - 4


def detour(energy):
    return energy - 4 if energy & 2 == 0 else energy + 4


def permute_energy(value, target_of, early=None):
    count = lax.axis_size("energy")
    pairs = [(source, target_of(source)) for source in range(count) if early is None or is_early(source) == early]
    return lax.ppermute(value, "energy", [(source, target) for source, target in pairs if 0 <= target < count])


def permute_mode(value, early):
    count, modes = lax.axis_size("energy"), lax.axis_size("mode")
    pairs = [
        (energy * modes + mode, energy * modes + other)
        for energy in range(count)
        if is_early(energy) == early
        for mode, other in SWAP
    ]
    return lax.ppermute(value, ("energy", "mode"), pairs)


def local_call(kernel, outputs, scalars, arrays):
    held = [pltpu.with_memory_space_constraint(each, pltpu.VMEM) for each in arrays]
    return pl.pallas_call(
        kernel,
        out_shape=[pltpu.VMEM(shape, dtype) for shape, dtype in outputs],
        in_specs=[SMEM] * len(scalars) + [VMEM] * len(held),
        out_specs=[VMEM] * len(outputs),
        compiler_params=LOCAL,
    )(*scalars, *held)


def own_mode():
    return lax.axis_index("mode")


def block(index, rows):
    return pl.ds(pl.multiple_of(index * rows, rows), rows)


def cut_kernel(columns, own_ref, *refs):
    pieces, sem = refs[:-1], refs[-1]
    copies = [
        pltpu.make_async_copy(own_ref.at[0, :, first:last], piece, sem.at[index])
        for index, ((first, last), piece) in enumerate(zip(columns, pieces))
    ]
    for copy in copies:
        copy.start()
    for copy in copies:
        copy.wait()


def cut(spectral, columns):
    return pl.pallas_call(
        functools.partial(cut_kernel, columns),
        out_shape=[pltpu.VMEM((spectral.shape[1], last - first), jnp.float32) for first, last in columns],
        in_specs=[ANY],
        out_specs=[VMEM] * len(columns),
        scratch_shapes=[pltpu.SemaphoreType.DMA((len(columns),))],
        compiler_params=LOCAL,
    )(spectral)


def merge_kernel(*refs):
    at = 0
    for piece in refs[:-1]:
        width = piece.shape[1]
        refs[-1][:, at : at + width] = piece[...]
        at += width


def merged(pieces):
    if len(pieces) == 1:
        return pieces[0]
    rows = pieces[0].shape[0]
    return local_call(merge_kernel, [((rows, sum(each.shape[1] for each in pieces)), jnp.float32)], [], pieces)[0]


def widened(matrix_ref, which, part):
    start = 2 * which + (lax.axis_index("energy") & 1)
    return matrix_ref[block(start, part), :].astype(jnp.float32)


def widen_kernel(offset_ref, level_ref, matrix_ref, out_ref):
    orbitals = matrix_ref.shape[0]
    part = orbitals // 4
    out_ref[0:part, :] = widened(matrix_ref, own_mode(), part)
    row = lax.broadcasted_iota(jnp.int32, (out_ref.shape[0] - part, orbitals), 0)
    out_ref[part:, :] = jnp.where(row == 0, offset_ref[0], level_ref[0, 0]).astype(out_ref.dtype)


def widen_more_kernel(matrix_ref, out_ref):
    out_ref[...] = widened(matrix_ref, 1 - own_mode(), out_ref.shape[0])


def take_columns(matrix_ref, out_ref):
    rows = out_ref.shape[1]

    @pl.when(own_mode() == 0)
    def _():
        out_ref[...] = matrix_ref[:, :rows]

    @pl.when(own_mode() != 0)
    def _():
        out_ref[...] = matrix_ref[:, rows:]


def columns_kernel(matrix_ref, near_ref, far_ref):
    rows = near_ref.shape[0]
    take_columns(matrix_ref.at[block(1 - own_mode(), rows), :], near_ref)
    take_columns(matrix_ref.at[block(own_mode(), rows), :], far_ref)


def join_rows(mine_ref, other_ref, out_ref):
    part = out_ref.shape[0] // 2
    core = lax.axis_index("energy") & 1
    out_ref[block(core, part), :] = mine_ref[0:part, :].astype(out_ref.dtype)
    out_ref[block(1 - core, part), :] = other_ref[0:part, :].astype(out_ref.dtype)


def join_kernel(mine_ref, other_ref, out_ref, left_ref):
    join_rows(mine_ref, other_ref, out_ref)
    take_columns(out_ref, left_ref)


def join_more_kernel(near_ref, mine_ref, other_ref, out_ref, left_ref):
    rows = near_ref.shape[0]
    out_ref[block(1 - own_mode(), rows), :] = near_ref[...]
    far = out_ref.at[block(own_mode(), rows), :]
    join_rows(mine_ref, other_ref, far)
    take_columns(far, left_ref)


def piece_view(refs, starts, first, last):
    for ref, start in zip(refs, starts):
        if start <= first and last <= start + ref.shape[1]:
            return ref[:, first - start : last - start]
    raise ValueError((first, last, starts))


def split_sources(refs, layout):
    split, at = [], 0
    for starts in layout:
        split.append((refs[at : at + len(starts)], starts))
        at += len(starts)
    return split


def combine(tiles, split, number, combined):
    energy = lax.axis_index("energy")
    step = 1 - 2 * (energy & 1)
    far = 2 - 4 * ((energy >> 1) & 1)
    told = number.shape[0] - 8
    offset, level = number[told : told + 1, 0:1], number[told + 1 : told + 2, 0:1]

    def weight(distance):
        gap = jnp.abs(distance).astype(jnp.float32)
        below = jnp.where(distance < 0, 1, 0).astype(jnp.float32)
        return jnp.where(offset == gap, level + below, 0.0)

    weights = [weight(distance) for distance in (step, far, -far, -step)]
    for first, last in tiles:
        total = None
        for (pieces, starts), factor in zip(split, weights):
            term = piece_view(pieces, starts, first, last) * factor
            total = term if total is None else total + term
        combined[:, first - tiles[0][0] : last - tiles[0][0]] = total.astype(jnp.bfloat16)


def left_kernel(tiles, layout, early, number, left, *refs):
    out, combined = refs[-2:]

    @pl.when(is_early(lax.axis_index("energy")) == early)
    def _():
        combine(tiles, split_sources(refs, layout), number, combined)
        out[...] = jnp.dot(left[...], combined[...], preferred_element_type=jnp.float32).astype(jnp.bfloat16)


def left_send_kernel(tiles, layout, early, scale, before, own_ref, near_ref, *refs):
    numbers, lefts, refs = refs[:2], refs[2:4], refs[4:]
    done, refs = refs[: 2 * len(before)], refs[2 * len(before) :]
    out_ref, outs, combined = refs[-5], refs[-4:-2], refs[-2:]

    @pl.when(is_early(lax.axis_index("energy")) == early)
    def _():
        pieces = []
        for mode in range(2):
            combine(tiles, split_sources(refs, layout), numbers[mode], combined[mode])
            product = jnp.dot(lefts[mode][...], combined[mode][...], preferred_element_type=jnp.float32)
            product = product.astype(jnp.bfloat16)
            outs[mode][...] = product
            pieces.append([each[...] for each in done[mode * len(before) : (mode + 1) * len(before)]] + [product])
        columns = [*before, (tiles[0][0], tiles[-1][1])]
        out_ref[...] = right_product(send_couplings(0, own_ref, near_ref, out_ref), pieces, columns) * scale


def right_product(couplings, pieces, columns):
    total = None
    for coupling, lefts in zip(couplings, pieces):
        for left, (first, last) in zip(lefts, columns):
            term = lax.dot_general(
                left, coupling[:, first:last], (((1,), (1,)), ((), ())), preferred_element_type=jnp.float32
            )
            total = term if total is None else total + term
    return total


def output_span(mode, index, rows, orbitals):
    whole = rows // LANES * LANES
    if index == 0:
        return mode * (orbitals - whole), whole
    return (1 - mode) * whole, orbitals - whole


def send_couplings(index, own_ref, other_ref, out_ref):
    orbitals, rows = own_ref.shape[0], out_ref.shape[0]
    target = 1 - own_mode()
    start, width = output_span(target, index, rows, orbitals)
    own = own_ref.at[pl.ds(pl.multiple_of(start, LANES), width), :]
    if other_ref.shape[0] == rows:
        start = start - target * rows
    return own, other_ref.at[pl.ds(pl.multiple_of(start, LANES // 2), width), :]


def send_kernel(scale, columns, early, own_ref, other_ref, *refs):
    pieces, out_ref = refs[:-1], refs[-1]
    many = len(columns)

    @pl.when(is_early(lax.axis_index("energy")) == early)
    def _():
        lefts = [[piece[...] for piece in pieces[mode * many : (mode + 1) * many]] for mode in range(2)]
        out_ref[...] = right_product(send_couplings(1, own_ref, other_ref, out_ref), lefts, columns) * scale


def keep_kernel(scale, variants, own_ref, other_ref, *refs):
    lefts, pieces, outs = refs[:2], refs[2:-2], refs[-2:]
    orbitals = own_ref.shape[0]
    at = 0
    for early, columns in variants:
        many = len(columns)
        group = pieces[at : at + 2 * many]
        at += 2 * many

        @pl.when(is_early(lax.axis_index("energy")) == early)
        def _(group=group, many=many, columns=columns):
            held = [
                [
                    jnp.dot(left[...], piece[...], preferred_element_type=jnp.float32).astype(jnp.bfloat16)
                    for piece in group[mode * many : (mode + 1) * many]
                ]
                for mode, left in enumerate(lefts)
            ]
            for index, out_ref in enumerate(outs):
                start, width = output_span(own_mode(), index, out_ref.shape[0], orbitals)
                span = pl.ds(pl.multiple_of(start, LANES), width)
                couplings = (own_ref.at[span, :], other_ref.at[span, :])
                out_ref[...] = right_product(couplings, held, columns) * scale


def finish_kernel(index, *refs):
    kept_ref, early_ref, late_ref = refs[:3]
    out_ref, piece_ref, sem = refs[-3:]
    piece_ref[...] = kept_ref[...] + (early_ref[...] + late_ref[...])
    for mode in range(2):

        @pl.when(own_mode() == mode)
        def _(mode=mode):
            start, width = output_span(mode, index, out_ref.shape[1], out_ref.shape[2])
            copy = pltpu.make_async_copy(piece_ref, out_ref.at[0, :, start : start + width], sem)
            copy.start()
            copy.wait()


def finish(index, result, before, *arrays):
    held = [pltpu.with_memory_space_constraint(each, pltpu.VMEM) for each in arrays]
    return pl.pallas_call(
        functools.partial(finish_kernel, index),
        out_shape=result,
        in_specs=[VMEM] * len(held) + [ANY] * len(before),
        out_specs=ANY,
        scratch_shapes=[pltpu.VMEM(arrays[0].shape, arrays[0].dtype), pltpu.SemaphoreType.DMA],
        input_output_aliases={len(held): 0} if before else {},
        compiler_params=LOCAL,
        name="finish",
    )(*held, *before)


def shards(spectral, coupling, offsets, occupation):
    rows, orbitals = spectral.shape[1:]
    matrix = coupling[0]
    scale = 1.0 / lax.axis_size("mode")
    tiles = tiles_of(orbitals)
    many = len(tiles)
    sides = ((0, many - 2), (many - 2, many))
    seconds = ((0, 1), (1, many))

    own_piece = cut(spectral, tiles[:1])
    across_piece = [permute_energy(own_piece[0], across)]
    own_piece += cut(spectral, tiles[1:])
    for index in range(1, many):
        across_piece.append(permute_energy(own_piece[index], across))

    part = orbitals // 4
    (wide,) = local_call(widen_kernel, [((part + 8, orbitals), jnp.float32)], [offsets, occupation], [matrix])
    (wide_more,) = local_call(widen_more_kernel, [((part, orbitals), jnp.float32)], [], [matrix])
    told = lax.ppermute(wide, "mode", SWAP)
    told_more = lax.ppermute(wide_more, "mode", SWAP)
    swapped = permute_energy(told, partner)
    swapped_more = permute_energy(told_more, partner)
    partner_piece = permute_energy(spectral[0], partner)

    first_piece = []
    for index in range(many - 1):
        first_piece.append(permute_energy(across_piece[index], onward, early=1))
    aside = permute_energy(own_piece[-1], detour, early=0)
    first_piece.append(permute_energy(aside, across, early=0))
    second_piece = []
    for low, high in seconds:
        second_piece.append(permute_energy(merged(across_piece[low:high]), onward, early=0))
    straight_piece = []
    for low, high in sides:
        straight_piece.append(permute_energy(merged(across_piece[low:high]), partner, early=0))
    crossed_piece = permute_energy(merged(first_piece), partner, early=1)

    square, strip = ((rows, rows), matrix.dtype), ((rows, orbitals), matrix.dtype)
    own_near_left, own_far_left = local_call(columns_kernel, [square] * 2, [], [matrix])
    near, near_left = local_call(join_kernel, [strip, square], [], [told, swapped])
    other_matrix, far_left = local_call(
        join_more_kernel, [(matrix.shape, matrix.dtype), square], [], [near, told_more, swapped_more]
    )

    starts = [first for first, last in tiles]
    widths = [output_span(0, index, rows, orbitals)[1] for index in range(2)]
    numbers, near_lefts = (wide, told), (own_near_left, near_left)
    ready, last = sides
    ready_columns, last_columns = [(tiles[low][0], tiles[high - 1][1]) for low, high in sides]

    def width(span):
        return span[1] - span[0]

    def left(which, low, high):
        layout = ([0], starts[low:high], starts[low:high], [starts[low]])
        return local_call(
            functools.partial(left_kernel, tiles[low:high], layout, 1),
            [((rows, width(ready_columns)), jnp.bfloat16)] * 2,
            [],
            [
                numbers[which], near_lefts[which], partner_piece,
                *across_piece[low:high], *first_piece[low:high], straight_piece[0],
            ],
        )

    def left_send(early, low, high, before, done, onward_pieces, onward_starts, back_piece):
        layout = ([0], starts[low:high], onward_starts, [starts[low]])
        wide_columns = tiles[high - 1][1] - tiles[low][0]
        return local_call(
            functools.partial(left_send_kernel, tiles[low:high], layout, early, scale, before),
            [((rows, widths[0]), jnp.float32)] + [((rows, wide_columns), jnp.bfloat16)] * 4,
            [],
            [
                matrix, near, *numbers, *near_lefts, *done, partner_piece,
                *across_piece[low:high], *onward_pieces, back_piece,
            ],
        )

    early_left = [left(which, *ready) for which in range(2)]
    early = left_send(
        1, *last, [ready_columns], [each for each, combined in early_left],
        first_piece[last[0] : last[1]], starts[last[0] : last[1]], straight_piece[1],
    )
    late = left_send(0, 0, many, [], [], second_piece, [starts[low] for low, high in seconds], crossed_piece)
    early_columns, late_columns = [ready_columns, last_columns], [(0, orbitals)]
    early_coupled = [early_left[0][0], early[1], early_left[1][0], early[2]]
    early_combined = [early_left[0][1], early[3], early_left[1][1], early[4]]
    late_coupled, late_combined = late[1:3], late[3:5]

    arrived = []
    for which, first_sent, columns, coupled in (
        (1, early[0], early_columns, early_coupled),
        (0, late[0], late_columns, late_coupled),
    ):
        got = [permute_mode(first_sent, which)]
        (sent,) = local_call(
            functools.partial(send_kernel, scale, columns, which),
            [((rows, widths[1]), jnp.float32)],
            [],
            [matrix, other_matrix, *coupled],
        )
        got.append(permute_mode(sent, which))
        arrived.append(got)
    kept = local_call(
        functools.partial(keep_kernel, scale, ((1, early_columns), (0, late_columns))),
        [((rows, each), jnp.float32) for each in widths],
        [],
        [matrix, other_matrix, own_far_left, far_left, *early_combined, *late_combined],
    )

    shape = jax.ShapeDtypeStruct(spectral.shape, jnp.float32)
    result = []
    for index in range(2):
        result = [finish(index, shape, result, kept[index], arrived[0][index], arrived[1][index])]
    return result[0]


def solution(mesh):
    return jax.shard_map(
        shards,
        mesh=mesh,
        in_specs=(P("energy", "mode", None), P("mode", None, None), P("mode"), P("mode", "energy")),
        out_specs=P("energy", "mode", None),
        check_vma=False,
    )
```

```python
import functools

import jax
import jax.numpy as jnp
from jax import lax
from jax.experimental import pallas as pl
from jax.experimental.pallas import tpu as pltpu
from jax.sharding import PartitionSpec as P


ANY = pl.BlockSpec(memory_space=pl.ANY)
VMEM = pl.BlockSpec(memory_space=pltpu.VMEM)
SMEM = pl.BlockSpec(memory_space=pltpu.SMEM)
LOCAL = pltpu.CompilerParams(vmem_limit_bytes=12 * 2**20)
SWAP = [(0, 1), (1, 0)]
LANES = 128


def tiles_of(columns):
    tiles, first = [], 0
    while first < columns:
        last = min(columns, first + (2 * LANES if columns - first > 3 * LANES else LANES))
        tiles.append((first, last))
        first = last
    return tiles


def is_early(energy):
    return (energy ^ (energy >> 1)) & 1


def partner(energy):
    return energy ^ 1


def across(energy):
    return energy ^ 2


def onward(energy):
    return energy + 4 if energy & 2 == 0 else energy - 4


def detour(energy):
    return energy - 4 if energy & 2 == 0 else energy + 4


def permute_energy(value, target_of, early=None):
    count = lax.axis_size("energy")
    pairs = [(source, target_of(source)) for source in range(count) if early is None or is_early(source) == early]
    return lax.ppermute(value, "energy", [(source, target) for source, target in pairs if 0 <= target < count])


def permute_mode(value, early):
    count, modes = lax.axis_size("energy"), lax.axis_size("mode")
    pairs = [
        (energy * modes + mode, energy * modes + other)
        for energy in range(count)
        if is_early(energy) == early
        for mode, other in SWAP
    ]
    return lax.ppermute(value, ("energy", "mode"), pairs)


def local_call(kernel, outputs, scalars, arrays):
    held = [pltpu.with_memory_space_constraint(each, pltpu.VMEM) for each in arrays]
    return pl.pallas_call(
        kernel,
        out_shape=[pltpu.VMEM(shape, dtype) for shape, dtype in outputs],
        in_specs=[SMEM] * len(scalars) + [VMEM] * len(held),
        out_specs=[VMEM] * len(outputs),
        compiler_params=LOCAL,
    )(*scalars, *held)


def own_mode():
    return lax.axis_index("mode")


def block(index, rows):
    return pl.ds(pl.multiple_of(index * rows, rows), rows)


def cut_kernel(columns, own_ref, *refs):
    pieces, sem = refs[:-1], refs[-1]
    copies = [
        pltpu.make_async_copy(own_ref.at[0, :, first:last], piece, sem.at[index])
        for index, ((first, last), piece) in enumerate(zip(columns, pieces))
    ]
    for copy in copies:
        copy.start()
    for copy in copies:
        copy.wait()


def cut(spectral, columns):
    return pl.pallas_call(
        functools.partial(cut_kernel, columns),
        out_shape=[pltpu.VMEM((spectral.shape[1], last - first), jnp.float32) for first, last in columns],
        in_specs=[ANY],
        out_specs=[VMEM] * len(columns),
        scratch_shapes=[pltpu.SemaphoreType.DMA((len(columns),))],
        compiler_params=LOCAL,
    )(spectral)


def merge_kernel(*refs):
    at = 0
    for piece in refs[:-1]:
        width = piece.shape[1]
        refs[-1][:, at : at + width] = piece[...]
        at += width


def merged(pieces):
    if len(pieces) == 1:
        return pieces[0]
    rows = pieces[0].shape[0]
    return local_call(merge_kernel, [((rows, sum(each.shape[1] for each in pieces)), jnp.float32)], [], pieces)[0]


def widened(matrix_ref, which, part):
    start = 2 * which + (lax.axis_index("energy") & 1)
    return matrix_ref[block(start, part), :].astype(jnp.float32)


def widen_kernel(offset_ref, level_ref, matrix_ref, out_ref):
    orbitals = matrix_ref.shape[0]
    part = orbitals // 4
    out_ref[0:part, :] = widened(matrix_ref, own_mode(), part)
    row = lax.broadcasted_iota(jnp.int32, (out_ref.shape[0] - part, orbitals), 0)
    out_ref[part:, :] = jnp.where(row == 0, offset_ref[0], level_ref[0, 0]).astype(out_ref.dtype)


def widen_more_kernel(matrix_ref, out_ref):
    out_ref[...] = widened(matrix_ref, 1 - own_mode(), out_ref.shape[0])


def take_columns(matrix_ref, out_ref):
    rows = out_ref.shape[1]

    @pl.when(own_mode() == 0)
    def _():
        out_ref[...] = matrix_ref[:, :rows]

    @pl.when(own_mode() != 0)
    def _():
        out_ref[...] = matrix_ref[:, rows:]


def columns_kernel(matrix_ref, near_ref, far_ref):
    rows = near_ref.shape[0]
    take_columns(matrix_ref.at[block(1 - own_mode(), rows), :], near_ref)
    take_columns(matrix_ref.at[block(own_mode(), rows), :], far_ref)


def join_rows(mine_ref, other_ref, out_ref):
    part = out_ref.shape[0] // 2
    core = lax.axis_index("energy") & 1
    out_ref[block(core, part), :] = mine_ref[0:part, :].astype(out_ref.dtype)
    out_ref[block(1 - core, part), :] = other_ref[0:part, :].astype(out_ref.dtype)


def join_kernel(mine_ref, other_ref, out_ref, left_ref):
    join_rows(mine_ref, other_ref, out_ref)
    take_columns(out_ref, left_ref)


def join_more_kernel(near_ref, mine_ref, other_ref, out_ref, left_ref):
    rows = near_ref.shape[0]
    out_ref[block(1 - own_mode(), rows), :] = near_ref[...]
    far = out_ref.at[block(own_mode(), rows), :]
    join_rows(mine_ref, other_ref, far)
    take_columns(far, left_ref)


def piece_view(refs, starts, first, last):
    for ref, start in zip(refs, starts):
        if start <= first and last <= start + ref.shape[1]:
            return ref[:, first - start : last - start]
    raise ValueError((first, last, starts))


def split_sources(refs, layout):
    split, at = [], 0
    for starts in layout:
        split.append((refs[at : at + len(starts)], starts))
        at += len(starts)
    return split


def combine(tiles, split, number, combined):
    energy = lax.axis_index("energy")
    step = 1 - 2 * (energy & 1)
    far = 2 - 4 * ((energy >> 1) & 1)
    told = number.shape[0] - 8
    offset, level = number[told : told + 1, 0:1], number[told + 1 : told + 2, 0:1]

    def weight(distance):
        gap = jnp.abs(distance).astype(jnp.float32)
        below = jnp.where(distance < 0, 1, 0).astype(jnp.float32)
        return jnp.where(offset == gap, level + below, 0.0)

    weights = [weight(distance) for distance in (step, far, -far, -step)]
    for first, last in tiles:
        total = None
        for (pieces, starts), factor in zip(split, weights):
            term = piece_view(pieces, starts, first, last) * factor
            total = term if total is None else total + term
        combined[:, first - tiles[0][0] : last - tiles[0][0]] = total.astype(jnp.bfloat16)


def left_kernel(tiles, layout, early, number, left, *refs):
    out, combined = refs[-2:]

    @pl.when(is_early(lax.axis_index("energy")) == early)
    def _():
        combine(tiles, split_sources(refs, layout), number, combined)
        out[...] = jnp.dot(left[...], combined[...], preferred_element_type=jnp.float32).astype(jnp.bfloat16)


def left_send_kernel(tiles, layout, early, scale, many, own_ref, near_ref, *refs):
    numbers, lefts, refs = refs[:2], refs[2:4], refs[4:]
    before, refs = refs[:many], refs[many:]
    out_ref, outs, combined = refs[-5], refs[-4:-2], refs[-2:]

    @pl.when(is_early(lax.axis_index("energy")) == early)
    def _():
        pieces = []
        for mode in range(2):
            combine(tiles, split_sources(refs, layout), numbers[mode], combined[mode])
            product = jnp.dot(lefts[mode][...], combined[mode][...], preferred_element_type=jnp.float32)
            product = product.astype(jnp.bfloat16)
            outs[mode][...] = product
            pieces.append([product])
        columns = [(tiles[0][0], tiles[-1][1])]
        total = right_product(send_couplings(0, own_ref, near_ref, out_ref), pieces, columns) * scale
        for each in before:
            total += each[...]
        out_ref[...] = total


def right_product(couplings, pieces, columns):
    total = None
    for coupling, lefts in zip(couplings, pieces):
        for left, (first, last) in zip(lefts, columns):
            term = lax.dot_general(
                left, coupling[:, first:last], (((1,), (1,)), ((), ())), preferred_element_type=jnp.float32
            )
            total = term if total is None else total + term
    return total


def output_span(mode, index, rows, orbitals):
    whole = rows // LANES * LANES
    if index == 0:
        return mode * (orbitals - whole), whole
    return (1 - mode) * whole, orbitals - whole


def send_couplings(index, own_ref, other_ref, out_ref):
    orbitals, rows = own_ref.shape[0], out_ref.shape[0]
    target = 1 - own_mode()
    start, width = output_span(target, index, rows, orbitals)
    own = own_ref.at[pl.ds(pl.multiple_of(start, LANES), width), :]
    if other_ref.shape[0] == rows:
        start = start - target * rows
    return own, other_ref.at[pl.ds(pl.multiple_of(start, LANES // 2), width), :]


def send_kernel(scale, columns, index, early, own_ref, other_ref, *refs):
    pieces, out_ref = refs[:-1], refs[-1]
    many = len(columns)

    @pl.when(is_early(lax.axis_index("energy")) == early)
    def _():
        lefts = [[piece[...] for piece in pieces[mode * many : (mode + 1) * many]] for mode in range(2)]
        out_ref[...] = right_product(send_couplings(index, own_ref, other_ref, out_ref), lefts, columns) * scale


def keep_kernel(scale, variants, own_ref, other_ref, *refs):
    lefts, pieces, outs = refs[:2], refs[2:-2], refs[-2:]
    orbitals = own_ref.shape[0]
    at = 0
    for early, columns in variants:
        many = len(columns)
        group = pieces[at : at + 2 * many]
        at += 2 * many

        @pl.when(is_early(lax.axis_index("energy")) == early)
        def _(group=group, many=many, columns=columns):
            held = [
                [
                    jnp.dot(left[...], piece[...], preferred_element_type=jnp.float32).astype(jnp.bfloat16)
                    for piece in group[mode * many : (mode + 1) * many]
                ]
                for mode, left in enumerate(lefts)
            ]
            for index, out_ref in enumerate(outs):
                start, width = output_span(own_mode(), index, out_ref.shape[0], orbitals)
                span = pl.ds(pl.multiple_of(start, LANES), width)
                couplings = (own_ref.at[span, :], other_ref.at[span, :])
                out_ref[...] = right_product(couplings, held, columns) * scale


def finish_kernel(index, *refs):
    kept_ref, early_ref, late_ref = refs[:3]
    out_ref, piece_ref, sem = refs[-3:]
    for mode in range(2):

        @pl.when(own_mode() == mode)
        def _(mode=mode):
            start, width = output_span(mode, index, out_ref.shape[1], out_ref.shape[2])
            copies = []
            for which, at in enumerate(range(0, width, LANES)):
                span = slice(at, at + LANES)
                piece_ref[:, span] = kept_ref[:, span] + (early_ref[:, span] + late_ref[:, span])
                target = out_ref.at[0, :, start + at : start + at + LANES]
                copies.append(pltpu.make_async_copy(piece_ref.at[:, span], target, sem.at[which]))
                copies[-1].start()
            for copy in copies:
                copy.wait()


def finish(index, result, before, *arrays):
    held = [pltpu.with_memory_space_constraint(each, pltpu.VMEM) for each in arrays]
    return pl.pallas_call(
        functools.partial(finish_kernel, index),
        out_shape=result,
        in_specs=[VMEM] * len(held) + [ANY] * len(before),
        out_specs=ANY,
        scratch_shapes=[
            pltpu.VMEM(arrays[0].shape, arrays[0].dtype),
            pltpu.SemaphoreType.DMA((arrays[0].shape[1] // LANES,)),
        ],
        input_output_aliases={len(held): 0} if before else {},
        compiler_params=LOCAL,
        name="finish",
    )(*held, *before)


def shards(spectral, coupling, offsets, occupation):
    rows, orbitals = spectral.shape[1:]
    matrix = coupling[0]
    scale = 1.0 / lax.axis_size("mode")
    tiles = tiles_of(orbitals)
    many = len(tiles)
    sides = ((0, many - 2), (many - 2, many))
    seconds = ((0, 1), (1, many))

    own_piece = cut(spectral, tiles[:1])
    across_piece = [permute_energy(own_piece[0], across)]
    own_piece += cut(spectral, tiles[1:])
    for index in range(1, many):
        across_piece.append(permute_energy(own_piece[index], across))

    part = orbitals // 4
    (wide,) = local_call(widen_kernel, [((part + 8, orbitals), jnp.float32)], [offsets, occupation], [matrix])
    (wide_more,) = local_call(widen_more_kernel, [((part, orbitals), jnp.float32)], [], [matrix])
    told = lax.ppermute(wide, "mode", SWAP)
    told_more = lax.ppermute(wide_more, "mode", SWAP)
    swapped = permute_energy(told, partner)
    swapped_more = permute_energy(told_more, partner)
    partner_piece = permute_energy(spectral[0], partner)

    first_piece = []
    for index in range(many - 1):
        first_piece.append(permute_energy(across_piece[index], onward, early=1))
    aside = permute_energy(own_piece[-1], detour, early=0)
    first_piece.append(permute_energy(aside, across, early=0))
    second_piece = []
    for low, high in seconds:
        second_piece.append(permute_energy(merged(across_piece[low:high]), onward, early=0))
    straight_piece = []
    for low, high in sides:
        straight_piece.append(permute_energy(merged(across_piece[low:high]), partner, early=0))
    crossed_piece = permute_energy(merged(first_piece), partner, early=1)

    square, strip = ((rows, rows), matrix.dtype), ((rows, orbitals), matrix.dtype)
    own_near_left, own_far_left = local_call(columns_kernel, [square] * 2, [], [matrix])
    near, near_left = local_call(join_kernel, [strip, square], [], [told, swapped])
    other_matrix, far_left = local_call(
        join_more_kernel, [(matrix.shape, matrix.dtype), square], [], [near, told_more, swapped_more]
    )

    starts = [first for first, last in tiles]
    widths = [output_span(0, index, rows, orbitals)[1] for index in range(2)]
    numbers, near_lefts = (wide, told), (own_near_left, near_left)
    ready, last = sides
    ready_columns, last_columns = [(tiles[low][0], tiles[high - 1][1]) for low, high in sides]

    def left(early, which, low, high, onward_pieces, onward_starts, back_piece, back_start):
        layout = ([0], starts[low:high], onward_starts, [back_start])
        return local_call(
            functools.partial(left_kernel, tiles[low:high], layout, early),
            [((rows, tiles[high - 1][1] - tiles[low][0]), jnp.bfloat16)] * 2,
            [],
            [
                numbers[which], near_lefts[which], partner_piece,
                *across_piece[low:high], *onward_pieces, back_piece,
            ],
        )

    def ahead(early, columns, coupled):
        return local_call(
            functools.partial(send_kernel, scale, [columns], 0, early),
            [((rows, widths[0]), jnp.float32)],
            [],
            [matrix, near, *coupled],
        )

    def left_send(early, low, high, before, onward_pieces, onward_starts, back_piece, back_start):
        layout = ([0], starts[low:high], onward_starts, [back_start])
        wide_columns = tiles[high - 1][1] - tiles[low][0]
        return local_call(
            functools.partial(left_send_kernel, tiles[low:high], layout, early, scale, len(before)),
            [((rows, widths[0]), jnp.float32)] + [((rows, wide_columns), jnp.bfloat16)] * 4,
            [],
            [
                matrix, near, *numbers, *near_lefts, *before, partner_piece,
                *across_piece[low:high], *onward_pieces, back_piece,
            ],
        )

    early_left = [
        left(1, which, *ready, first_piece[ready[0] : ready[1]], starts[ready[0] : ready[1]], straight_piece[0], 0)
        for which in range(2)
    ]
    early = left_send(
        1, *last, ahead(1, ready_columns, [each for each, combined in early_left]),
        first_piece[last[0] : last[1]], starts[last[0] : last[1]], straight_piece[1], starts[last[0]],
    )
    late_left = [left(0, which, 0, 1, second_piece[:1], [0], crossed_piece, 0) for which in range(2)]
    late = left_send(
        0, 1, many, ahead(0, tiles[0], [each for each, combined in late_left]),
        second_piece[1:], [starts[low] for low, high in seconds[1:]], crossed_piece, 0,
    )
    early_columns, late_columns = [ready_columns, last_columns], [tiles[0], (starts[1], orbitals)]
    early_coupled, early_combined, late_coupled, late_combined = (
        [early_left[0][which], early[1 + 2 * which], early_left[1][which], early[2 + 2 * which]]
        if group == 1
        else [late_left[0][which], late[1 + 2 * which], late_left[1][which], late[2 + 2 * which]]
        for group in (1, 0)
        for which in range(2)
    )

    arrived = []
    for which, first_sent, columns, coupled in (
        (1, early[0], early_columns, early_coupled),
        (0, late[0], late_columns, late_coupled),
    ):
        got = [permute_mode(first_sent, which)]
        (sent,) = local_call(
            functools.partial(send_kernel, scale, columns, 1, which),
            [((rows, widths[1]), jnp.float32)],
            [],
            [matrix, other_matrix, *coupled],
        )
        got.append(permute_mode(sent, which))
        arrived.append(got)
    kept = local_call(
        functools.partial(keep_kernel, scale, ((1, early_columns), (0, late_columns))),
        [((rows, each), jnp.float32) for each in widths],
        [],
        [matrix, other_matrix, own_far_left, far_left, *early_combined, *late_combined],
    )

    shape = jax.ShapeDtypeStruct(spectral.shape, jnp.float32)
    result = []
    for index in range(2):
        result = [finish(index, shape, result, kept[index], arrived[0][index], arrived[1][index])]
    return result[0]


def solution(mesh):
    return jax.shard_map(
        shards,
        mesh=mesh,
        in_specs=(P("energy", "mode", None), P("mode", None, None), P("mode"), P("mode", "energy")),
        out_specs=P("energy", "mode", None),
        check_vma=False,
    )
```

```python
import functools

import jax
import jax.numpy as jnp
from jax import lax
from jax.experimental import pallas as pl
from jax.experimental.pallas import tpu as pltpu
from jax.sharding import PartitionSpec as P


ANY = pl.BlockSpec(memory_space=pl.ANY)
VMEM = pl.BlockSpec(memory_space=pltpu.VMEM)
SMEM = pl.BlockSpec(memory_space=pltpu.SMEM)
LOCAL = pltpu.CompilerParams(vmem_limit_bytes=12 * 2**20)
SWAP = [(0, 1), (1, 0)]
LANES = 128


def tiles_of(columns):
    tiles, first = [], 0
    while first < columns:
        last = min(columns, first + (2 * LANES if columns - first > 3 * LANES else LANES))
        tiles.append((first, last))
        first = last
    return tiles


def is_early(energy):
    return (energy ^ (energy >> 1)) & 1


def partner(energy):
    return energy ^ 1


def across(energy):
    return energy ^ 2


def onward(energy):
    return energy + 4 if energy & 2 == 0 else energy - 4


def detour(energy):
    return energy - 4 if energy & 2 == 0 else energy + 4


def permute_energy(value, target_of, early=None):
    count = lax.axis_size("energy")
    pairs = [(source, target_of(source)) for source in range(count) if early is None or is_early(source) == early]
    return lax.ppermute(value, "energy", [(source, target) for source, target in pairs if 0 <= target < count])


def permute_mode(value, early):
    count, modes = lax.axis_size("energy"), lax.axis_size("mode")
    pairs = [
        (energy * modes + mode, energy * modes + other)
        for energy in range(count)
        if is_early(energy) == early
        for mode, other in SWAP
    ]
    return lax.ppermute(value, ("energy", "mode"), pairs)


def local_call(kernel, outputs, scalars, arrays):
    held = [pltpu.with_memory_space_constraint(each, pltpu.VMEM) for each in arrays]
    return pl.pallas_call(
        kernel,
        out_shape=[pltpu.VMEM(shape, dtype) for shape, dtype in outputs],
        in_specs=[SMEM] * len(scalars) + [VMEM] * len(held),
        out_specs=[VMEM] * len(outputs),
        compiler_params=LOCAL,
    )(*scalars, *held)


def own_mode():
    return lax.axis_index("mode")


def block(index, rows):
    return pl.ds(pl.multiple_of(index * rows, rows), rows)


def cut_kernel(columns, own_ref, *refs):
    pieces, sem = refs[:-1], refs[-1]
    copies = [
        pltpu.make_async_copy(own_ref.at[0, :, first:last], piece, sem.at[index])
        for index, ((first, last), piece) in enumerate(zip(columns, pieces))
    ]
    for copy in copies:
        copy.start()
    for copy in copies:
        copy.wait()


def cut(spectral, columns):
    return pl.pallas_call(
        functools.partial(cut_kernel, columns),
        out_shape=[pltpu.VMEM((spectral.shape[1], last - first), jnp.float32) for first, last in columns],
        in_specs=[ANY],
        out_specs=[VMEM] * len(columns),
        scratch_shapes=[pltpu.SemaphoreType.DMA((len(columns),))],
        compiler_params=LOCAL,
    )(spectral)


def merge_kernel(*refs):
    at = 0
    for piece in refs[:-1]:
        width = piece.shape[1]
        refs[-1][:, at : at + width] = piece[...]
        at += width


def merged(pieces):
    if len(pieces) == 1:
        return pieces[0]
    rows = pieces[0].shape[0]
    return local_call(merge_kernel, [((rows, sum(each.shape[1] for each in pieces)), jnp.float32)], [], pieces)[0]


def widened(matrix_ref, which, part):
    start = 2 * which + (lax.axis_index("energy") & 1)
    return matrix_ref[block(start, part), :].astype(jnp.float32)


def widen_kernel(offset_ref, level_ref, matrix_ref, out_ref):
    orbitals = matrix_ref.shape[0]
    part = orbitals // 4
    out_ref[0:part, :] = widened(matrix_ref, own_mode(), part)
    row = lax.broadcasted_iota(jnp.int32, (out_ref.shape[0] - part, orbitals), 0)
    out_ref[part:, :] = jnp.where(row == 0, offset_ref[0], level_ref[0, 0]).astype(out_ref.dtype)


def widen_more_kernel(matrix_ref, out_ref):
    out_ref[...] = widened(matrix_ref, 1 - own_mode(), out_ref.shape[0])


def take_columns(matrix_ref, out_ref):
    rows = out_ref.shape[1]

    @pl.when(own_mode() == 0)
    def _():
        out_ref[...] = matrix_ref[:, :rows]

    @pl.when(own_mode() != 0)
    def _():
        out_ref[...] = matrix_ref[:, rows:]


def columns_kernel(matrix_ref, near_ref, far_ref):
    rows = near_ref.shape[0]
    take_columns(matrix_ref.at[block(1 - own_mode(), rows), :], near_ref)
    take_columns(matrix_ref.at[block(own_mode(), rows), :], far_ref)


def join_rows(mine_ref, other_ref, out_ref):
    part = out_ref.shape[0] // 2
    core = lax.axis_index("energy") & 1
    out_ref[block(core, part), :] = mine_ref[0:part, :].astype(out_ref.dtype)
    out_ref[block(1 - core, part), :] = other_ref[0:part, :].astype(out_ref.dtype)


def join_kernel(mine_ref, other_ref, out_ref, left_ref):
    join_rows(mine_ref, other_ref, out_ref)
    take_columns(out_ref, left_ref)


def join_more_kernel(near_ref, mine_ref, other_ref, out_ref, left_ref):
    rows = near_ref.shape[0]
    out_ref[block(1 - own_mode(), rows), :] = near_ref[...]
    far = out_ref.at[block(own_mode(), rows), :]
    join_rows(mine_ref, other_ref, far)
    take_columns(far, left_ref)


def piece_view(refs, starts, first, last):
    for ref, start in zip(refs, starts):
        if start <= first and last <= start + ref.shape[1]:
            return ref[:, first - start : last - start]
    raise ValueError((first, last, starts))


def split_sources(refs, layout):
    split, at = [], 0
    for starts in layout:
        split.append((refs[at : at + len(starts)], starts))
        at += len(starts)
    return split


def combine(tiles, split, number, combined):
    energy = lax.axis_index("energy")
    step = 1 - 2 * (energy & 1)
    far = 2 - 4 * ((energy >> 1) & 1)
    told = number.shape[0] - 8
    offset, level = number[told : told + 1, 0:1], number[told + 1 : told + 2, 0:1]

    def weight(distance):
        gap = jnp.abs(distance).astype(jnp.float32)
        below = jnp.where(distance < 0, 1, 0).astype(jnp.float32)
        return jnp.where(offset == gap, level + below, 0.0)

    weights = [weight(distance) for distance in (step, far, -far, -step)]
    for first, last in tiles:
        total = None
        for (pieces, starts), factor in zip(split, weights):
            term = piece_view(pieces, starts, first, last) * factor
            total = term if total is None else total + term
        combined[:, first - tiles[0][0] : last - tiles[0][0]] = total.astype(jnp.bfloat16)


def left_send_kernel(tiles, layout, early, scale, many, own_ref, near_ref, *refs):
    numbers, lefts, refs = refs[:2], refs[2:4], refs[4:]
    before, refs = refs[:many], refs[many:]
    out_ref, outs, combined = refs[-5], refs[-4:-2], refs[-2:]

    @pl.when(is_early(lax.axis_index("energy")) == early)
    def _():
        pieces = []
        for mode in range(2):
            combine(tiles, split_sources(refs, layout), numbers[mode], combined[mode])
            product = jnp.dot(lefts[mode][...], combined[mode][...], preferred_element_type=jnp.float32)
            product = product.astype(jnp.bfloat16)
            outs[mode][...] = product
            pieces.append([product])
        columns = [(tiles[0][0], tiles[-1][1])]
        total = right_product(send_couplings(0, own_ref, near_ref, out_ref), pieces, columns) * scale
        for each in before:
            total += each[...]
        out_ref[...] = total


def right_product(couplings, pieces, columns):
    total = None
    for coupling, lefts in zip(couplings, pieces):
        for left, (first, last) in zip(lefts, columns):
            term = lax.dot_general(
                left, coupling[:, first:last], (((1,), (1,)), ((), ())), preferred_element_type=jnp.float32
            )
            total = term if total is None else total + term
    return total


def output_span(mode, index, rows, orbitals):
    whole = rows // LANES * LANES
    if index == 0:
        return mode * (orbitals - whole), whole
    return (1 - mode) * whole, orbitals - whole


def send_couplings(index, own_ref, other_ref, out_ref):
    orbitals, rows = own_ref.shape[0], out_ref.shape[0]
    target = 1 - own_mode()
    start, width = output_span(target, index, rows, orbitals)
    own = own_ref.at[pl.ds(pl.multiple_of(start, LANES), width), :]
    if other_ref.shape[0] == rows:
        start = start - target * rows
    return own, other_ref.at[pl.ds(pl.multiple_of(start, LANES // 2), width), :]


def send_kernel(scale, columns, index, early, own_ref, other_ref, *refs):
    pieces, out_ref = refs[:-1], refs[-1]
    many = len(columns)

    @pl.when(is_early(lax.axis_index("energy")) == early)
    def _():
        lefts = [[piece[...] for piece in pieces[mode * many : (mode + 1) * many]] for mode in range(2)]
        out_ref[...] = right_product(send_couplings(index, own_ref, other_ref, out_ref), lefts, columns) * scale


def keep_kernel(scale, variants, own_ref, other_ref, *refs):
    lefts, pieces, outs = refs[:2], refs[2:-2], refs[-2:]
    orbitals = own_ref.shape[0]
    at = 0
    for early, columns in variants:
        many = len(columns)
        group = pieces[at : at + 2 * many]
        at += 2 * many

        @pl.when(is_early(lax.axis_index("energy")) == early)
        def _(group=group, many=many, columns=columns):
            held = [
                [
                    jnp.dot(left[...], piece[...], preferred_element_type=jnp.float32).astype(jnp.bfloat16)
                    for piece in group[mode * many : (mode + 1) * many]
                ]
                for mode, left in enumerate(lefts)
            ]
            for index, out_ref in enumerate(outs):
                start, width = output_span(own_mode(), index, out_ref.shape[0], orbitals)
                span = pl.ds(pl.multiple_of(start, LANES), width)
                couplings = (own_ref.at[span, :], other_ref.at[span, :])
                out_ref[...] = right_product(couplings, held, columns) * scale


def finish_kernel(index, *refs):
    kept_ref, early_ref, late_ref = refs[:3]
    out_ref, piece_ref, sem = refs[-3:]
    for mode in range(2):

        @pl.when(own_mode() == mode)
        def _(mode=mode):
            start, width = output_span(mode, index, out_ref.shape[1], out_ref.shape[2])
            copies = []
            for which, at in enumerate(range(0, width, LANES)):
                span = slice(at, at + LANES)
                piece_ref[:, span] = kept_ref[:, span] + (early_ref[:, span] + late_ref[:, span])
                target = out_ref.at[0, :, start + at : start + at + LANES]
                copies.append(pltpu.make_async_copy(piece_ref.at[:, span], target, sem.at[which]))
                copies[-1].start()
            for copy in copies:
                copy.wait()


def finish(index, result, before, *arrays):
    held = [pltpu.with_memory_space_constraint(each, pltpu.VMEM) for each in arrays]
    return pl.pallas_call(
        functools.partial(finish_kernel, index),
        out_shape=result,
        in_specs=[VMEM] * len(held) + [ANY] * len(before),
        out_specs=ANY,
        scratch_shapes=[
            pltpu.VMEM(arrays[0].shape, arrays[0].dtype),
            pltpu.SemaphoreType.DMA((arrays[0].shape[1] // LANES,)),
        ],
        input_output_aliases={len(held): 0} if before else {},
        compiler_params=LOCAL,
        name="finish",
    )(*held, *before)


def shards(spectral, coupling, offsets, occupation):
    rows, orbitals = spectral.shape[1:]
    matrix = coupling[0]
    scale = 1.0 / lax.axis_size("mode")
    tiles = tiles_of(orbitals)
    many = len(tiles)
    sides = ((0, many - 2), (many - 2, many))
    seconds = ((0, 1), (1, many))

    own_piece = cut(spectral, tiles[:1])
    across_piece = [permute_energy(own_piece[0], across)]
    own_piece += cut(spectral, tiles[1:])
    for index in range(1, many):
        across_piece.append(permute_energy(own_piece[index], across))

    part = orbitals // 4
    (wide,) = local_call(widen_kernel, [((part + 8, orbitals), jnp.float32)], [offsets, occupation], [matrix])
    (wide_more,) = local_call(widen_more_kernel, [((part, orbitals), jnp.float32)], [], [matrix])
    told = lax.ppermute(wide, "mode", SWAP)
    told_more = lax.ppermute(wide_more, "mode", SWAP)
    swapped = permute_energy(told, partner)
    swapped_more = permute_energy(told_more, partner)
    partner_piece = permute_energy(spectral[0], partner)

    first_piece = []
    for index in range(many - 1):
        first_piece.append(permute_energy(across_piece[index], onward, early=1))
    aside = permute_energy(own_piece[-1], detour, early=0)
    first_piece.append(permute_energy(aside, across, early=0))
    second_piece = []
    for low, high in seconds:
        second_piece.append(permute_energy(merged(across_piece[low:high]), onward, early=0))
    straight_piece = []
    for low, high in sides:
        straight_piece.append(permute_energy(merged(across_piece[low:high]), partner, early=0))
    crossed_piece = permute_energy(merged(first_piece), partner, early=1)

    square, strip = ((rows, rows), matrix.dtype), ((rows, orbitals), matrix.dtype)
    own_near_left, own_far_left = local_call(columns_kernel, [square] * 2, [], [matrix])
    near, near_left = local_call(join_kernel, [strip, square], [], [told, swapped])
    other_matrix, far_left = local_call(
        join_more_kernel, [(matrix.shape, matrix.dtype), square], [], [near, told_more, swapped_more]
    )

    starts = [first for first, last in tiles]
    widths = [output_span(0, index, rows, orbitals)[1] for index in range(2)]
    numbers, near_lefts = (wide, told), (own_near_left, near_left)
    ready, last = sides
    ready_columns, last_columns = [(tiles[low][0], tiles[high - 1][1]) for low, high in sides]

    def left_send(early, low, high, before, onward_pieces, onward_starts, back_piece, back_start):
        layout = ([0], starts[low:high], onward_starts, [back_start])
        wide_columns = tiles[high - 1][1] - tiles[low][0]
        return local_call(
            functools.partial(left_send_kernel, tiles[low:high], layout, early, scale, len(before)),
            [((rows, widths[0]), jnp.float32)] + [((rows, wide_columns), jnp.bfloat16)] * 4,
            [],
            [
                matrix, near, *numbers, *near_lefts, *before, partner_piece,
                *across_piece[low:high], *onward_pieces, back_piece,
            ],
        )

    early_ahead = left_send(
        1, *ready, [], first_piece[ready[0] : ready[1]], starts[ready[0] : ready[1]], straight_piece[0], 0
    )
    early = left_send(
        1, *last, early_ahead[:1],
        first_piece[last[0] : last[1]], starts[last[0] : last[1]], straight_piece[1], starts[last[0]],
    )
    late_ahead = left_send(0, 0, 1, [], second_piece[:1], [0], crossed_piece, 0)
    late = left_send(
        0, 1, many, late_ahead[:1],
        second_piece[1:], [starts[low] for low, high in seconds[1:]], crossed_piece, 0,
    )
    early_columns, late_columns = [ready_columns, last_columns], [tiles[0], (starts[1], orbitals)]
    early_coupled, early_combined, late_coupled, late_combined = (
        [group[at + mode] for mode in range(2) for group in groups]
        for groups in ((early_ahead, early), (late_ahead, late))
        for at in (1, 3)
    )

    arrived = []
    for which, first_sent, columns, coupled in (
        (1, early[0], early_columns, early_coupled),
        (0, late[0], late_columns, late_coupled),
    ):
        got = [permute_mode(first_sent, which)]
        (sent,) = local_call(
            functools.partial(send_kernel, scale, columns, 1, which),
            [((rows, widths[1]), jnp.float32)],
            [],
            [matrix, other_matrix, *coupled],
        )
        got.append(permute_mode(sent, which))
        arrived.append(got)
    kept = local_call(
        functools.partial(keep_kernel, scale, ((1, early_columns), (0, late_columns))),
        [((rows, each), jnp.float32) for each in widths],
        [],
        [matrix, other_matrix, own_far_left, far_left, *early_combined, *late_combined],
    )

    shape = jax.ShapeDtypeStruct(spectral.shape, jnp.float32)
    result = []
    for index in range(2):
        result = [finish(index, shape, result, kept[index], arrived[0][index], arrived[1][index])]
    return result[0]


def solution(mesh):
    return jax.shard_map(
        shards,
        mesh=mesh,
        in_specs=(P("energy", "mode", None), P("mode", None, None), P("mode"), P("mode", "energy")),
        out_specs=P("energy", "mode", None),
        check_vma=False,
    )
```
